256 devices in a mesh: aperture: 4 (over x), tile: 64 (over y, z, core).
Axes of the slice: x: 4, y: 4, z: 8, core: 2. Of those that a mesh axis runs over, the one named last changes fastest.
Arguments:
- sectors: bfloat16 [4, 768, 512, 2, 512], P('aperture', 'tile'), may hold values from -6 to 6
- footprint: int32 [4, 768, 2], P('aperture', 'tile'), may hold values from 0 to 6, as said below
- own_blocks: bfloat16 [6, 512, 512], replicated, may hold values from -0.25 to 0.25
- edge_blocks: bfloat16 [6, 128, 512], replicated, may hold values from -0.25 to 0.25
- edges: int32 [512, 2], P(('aperture', 'tile')), may hold values from 0 to 32768, as said below
Outputs:
- image: float32 [2, 512, 32768], P(None, ('aperture', 'tile'))
The draws below stay inside these ranges and needn't reach their ends.
Inputs may be any that keep to these rules, and one draw needn't show every extreme that they name: `footprint`: per device, each group's 12 slots at one tile position hold first the live slots (own entry below 6), then dead ones with both entries 6; at least one slot is live; in every draw some device has all 12 slots live. The edge entry is 6 for every slot at the last tile position. `edges`: each interval spans at least 64 cells; in every draw some line starts at 0 and some line ends at 32768.
All inputs are finite; a program needn't handle non-finite values.
Results may differ from the reference program's by a relative error of at most 0.0003.
Values sent between devices are 32-bit elements; how exact they have to be, the bound alone decides.
No kernel may reach another device: no remote copies, remote signals or barrier semaphores. Data moves between devices by JAX's collectives and lax.ppermute only.
A program may use at most 128 MiB of HBM per device.

```python
import jax
import jax.numpy as jnp
from jax import lax

TK = 512
KY = 512
SK = 512
HB = 128
NB = 6
GORDER = 8
GMIN = 64
S_DEV = 12
GROUPS = 4
TILES = 64
SLOTS = 768
NX = 32768


def draw_footprint(key, part):
    keys = jax.random.split(key, 5)
    base = jax.random.randint(keys[0], (GROUPS, TILES), 1, 3)
    heavy = jax.random.randint(keys[1], (GROUPS, TILES), 0, 8) == 0
    chosen = jax.random.randint(keys[2], (), 0, GROUPS * TILES)
    device = jnp.arange(GROUPS * TILES, dtype=jnp.int32).reshape(GROUPS, TILES)
    live = jnp.where(heavy | (device == chosen), S_DEV, base)
    slot = jnp.arange(S_DEV, dtype=jnp.int32)
    alive = slot[None, None, :] < live[:, :, None]
    own = jax.random.randint(keys[3], (GROUPS, TILES, S_DEV), 0, NB)
    edge = jax.random.randint(keys[4], (GROUPS, TILES, S_DEV), 0, NB + 1)
    last = jnp.arange(TILES, dtype=jnp.int32)[None, :, None] == TILES - 1
    edge = jnp.where(last, NB, edge)
    own = jnp.where(alive, own, NB)
    edge = jnp.where(alive, edge, NB)
    return jnp.stack([own, edge], -1).reshape(GROUPS, TILES * S_DEV, 2).astype(jnp.int32)


def draw_edges(key, part):
    keys = jax.random.split(key, 4)
    span = jax.random.randint(keys[0], (KY,), GMIN, NX // 4 + 1)
    lower = jax.random.randint(keys[1], (KY,), 0, NX) % (NX - span + 1)
    first = jax.random.randint(keys[2], (), 0, KY)
    second = (first + 1 + jax.random.randint(keys[3], (), 0, KY - 1)) % KY
    rows = jnp.arange(KY, dtype=jnp.int32)
    lower = jnp.where(rows == first, 0, lower)
    lower = jnp.where(rows == second, NX - span, lower)
    return jnp.stack([lower, lower + span], -1).astype(jnp.int32)


def block_levels(rng, shape, shards, low, top_value):
    level, own = 1.0, jax.random.fold_in(rng, 6)
    for axis_at, shards_of in shards:
        draws = jnp.exp(jax.random.uniform(jax.random.fold_in(own, axis_at), (shards_of,), jnp.float32, low / len(shards), top_value / len(shards)))
        level = level * jnp.repeat(draws, shape[axis_at] // shards_of).reshape([-1 if axis == axis_at else 1 for axis in range(len(shape))])
    return level


def centred(key, shape, scale, limit, shards=(), kind=jnp.bfloat16):
    drawn = jax.random.normal(key, shape, jnp.float32) * scale
    if len(shards) > 0:
        drawn = block_levels(key, shape, shards, -0.22, 0.18) * drawn
    return jnp.clip(drawn, min=-limit, max=limit).astype(kind)


def setup_inputs(seed: int = 0) -> dict:
    key_list = jax.random.split(jax.random.key(seed), 6)
    sectors = centred(key_list[0], (GROUPS, SLOTS, SK, 2, KY), 1.0, 6.0, ((0, 4), (1, 64)))
    footprint = draw_footprint(jax.random.fold_in(key_list[5], 71), 0)
    own_blocks = centred(key_list[2], (NB, TK, SK), SK ** -0.5, 0.25)
    edge_blocks = centred(key_list[3], (NB, HB, SK), SK ** -0.5, 0.25)
    edges = draw_edges(jax.random.fold_in(key_list[5], 71), 0)
    return {"sectors": sectors, "footprint": footprint, "own_blocks": own_blocks, "edge_blocks": edge_blocks, "edges": edges}


def gegen_fix(field, edges):
    width = field.shape[-1]
    cells = jnp.arange(width, dtype=jnp.int32)[None, :]
    lower = edges[:, 0:1]
    upper = edges[:, 1:2]
    span = (upper - lower).astype(jnp.float32)
    inside = (cells >= lower) & (cells < upper)
    offset = (cells - lower).astype(jnp.float32)
    xi_vals = jnp.where(inside, -1.0 + (2.0 * offset + 1.0) / span, 0.0)
    base = 1.0 - xi_vals * xi_vals
    weight = jnp.where(inside, base * jnp.sqrt(base), 0.0)
    prev = jnp.ones_like(xi_vals)
    curr = 4.0 * xi_vals
    rebuilt = jnp.zeros_like(field)
    for order in range(GORDER):
        poly = prev if order == 0 else curr
        numer = lax.optimization_barrier(jnp.sum(weight * poly * field, axis=-1))
        denom = lax.optimization_barrier(jnp.sum(weight * poly * poly, axis=-1))
        rebuilt = rebuilt + (numer / denom)[..., None] * poly
        if order >= 1:
            nxt = (2.0 * (order + 2) * xi_vals * curr - (order + 3) * prev) / (order + 1)
            prev, curr = (curr, nxt)
    return jnp.where(inside, rebuilt, field)

def slot_terms(data, foot, own_f, edge_f):
    dims = (((0,), (1,)), ((), ()))

    def step(carry, item):
        total, rim = carry
        block, entry = item
        values = block.astype(jnp.float32)

        def own_term():
            kernel = own_f[jnp.minimum(entry[0], NB - 1)]
            return lax.dot_general(values, kernel, dims, precision=lax.Precision.HIGHEST)

        def edge_term():
            kernel = edge_f[jnp.minimum(entry[1], NB - 1)]
            return lax.dot_general(values, kernel, dims, precision=lax.Precision.HIGHEST)
        total = total + lax.cond(entry[0] < NB, own_term, lambda: jnp.zeros_like(total))
        rim = rim + lax.cond(entry[1] < NB, edge_term, lambda: jnp.zeros_like(rim))
        return ((total, rim), None)
    start = (jnp.zeros((2, KY, TK), jnp.float32), jnp.zeros((2, KY, HB), jnp.float32))
    (total, rim), _ = lax.scan(step, start, (data, foot))
    return (total, rim)

def reference(sectors, footprint, own_blocks, edge_blocks, edges):
    own_f = own_blocks.astype(jnp.float32)
    edge_f = edge_blocks.astype(jnp.float32)
    zero = jnp.zeros((), jnp.int32)

    def visit(flat, grid):
        group = (flat // TILES).astype(jnp.int32)
        place = (flat % TILES).astype(jnp.int32)
        data = lax.dynamic_slice(sectors, (group, place * S_DEV, zero, zero, zero), (1, S_DEV, SK, 2, KY))[0]
        foot = lax.dynamic_slice(footprint, (group, place * S_DEV, zero), (1, S_DEV, 2))[0]
        total, rim = slot_terms(data, foot, own_f, edge_f)
        begin = (place * TK).astype(jnp.int32)
        current = lax.dynamic_slice(grid, (zero, zero, begin), (2, KY, TK))
        grid = lax.dynamic_update_slice(grid, current + total, (zero, zero, begin))
        after = (begin + TK).astype(jnp.int32)
        current = lax.dynamic_slice(grid, (zero, zero, after), (2, KY, HB))
        grid = lax.dynamic_update_slice(grid, current + rim, (zero, zero, after))
        return grid
    grid = jnp.zeros((2, KY, NX + HB), jnp.float32)
    grid = lax.fori_loop(0, GROUPS * TILES, visit, grid)
    grid = grid[:, :, :NX]
    spectrum = lax.complex(grid[0], grid[1])
    pixels = jnp.fft.ifft(spectrum, axis=-1, norm='ortho')
    field = jnp.stack([jnp.real(pixels), jnp.imag(pixels)]).astype(jnp.float32)
    return gegen_fix(field, edges)
```

```python
import functools
import math

import jax
import jax.numpy as jnp
import numpy as np
from jax import lax
from jax.experimental import pallas as pl
from jax.experimental.pallas import tpu as pltpu
from jax.sharding import PartitionSpec as P

GORDER = 8
LANES = 128
f32, bf16 = jnp.float32, jnp.bfloat16


def vmem():
    return pl.BlockSpec(memory_space=pltpu.VMEM)


def position(part, relative):
    return (relative - 1) & 3 if part == 0 else 3 - relative


def slot_kernel(cfg, foot, x_hbm, own_hbm, edge_hbm, low_ref, high_ref, rim_ref, xs, owns, edges, wide0, wide1, sems, bsem):
    slots, blocks, rows, erows = cfg
    me = lax.axis_index("aperture")
    depth = x_hbm.shape[1] // 8
    count = jnp.int32(0)
    for s in range(slots):
        count = count + (foot[2 * s] < blocks).astype(jnp.int32)

    def fetch(s):
        return pltpu.make_async_copy(x_hbm.at[s], xs.at[s], sems.at[s])

    own_copy = pltpu.make_async_copy(own_hbm, owns, bsem.at[0])
    edge_copy = pltpu.make_async_copy(edge_hbm, edges, bsem.at[1])
    fetch(0).start()
    own_copy.start()
    edge_copy.start()
    for s in range(1, slots):
        @pl.when(s < count)
        def _():
            fetch(s).start()
    low_ref[...] = jnp.zeros_like(low_ref)
    high_ref[...] = jnp.zeros_like(high_ref)
    rim_ref[...] = jnp.zeros_like(rim_ref)

    def widen(s, wide):
        wide[...] = xs[s].astype(f32)

    def multiply(s, wide):
        e = foot[2 * s + 1]
        keep = (e < blocks).astype(bf16)
        kern = jnp.concatenate([owns[foot[2 * s]], edges[jnp.minimum(e, blocks - 1)] * keep], axis=0)
        for p in range(2):
            x = jnp.concatenate(
                [wide[pl.ds(2 * j + p, depth, stride=8), :].astype(bf16) for j in range(4)], axis=1
            )
            y = jnp.dot(kern, x, preferred_element_type=f32)
            for d in range(4):
                pos = position(p, me ^ d)
                part = y[:, d * LANES:(d + 1) * LANES]
                low_ref[p, pos] += part[:erows]
                high_ref[p, pos] += part[erows:rows]
                rim_ref[p, pos] += part[rows:]

    fetch(0).wait()
    widen(0, wide0)
    own_copy.wait()
    edge_copy.wait()

    def step(s, here, there):
        @pl.when(s + 1 < count)
        def _():
            fetch(s + 1).wait()
        widen(jnp.minimum(s + 1, count - 1), there)
        multiply(s, here)

    def pair(t, carry):
        step(2 * t, wide0, wide1)

        @pl.when(2 * t + 1 < count)
        def _():
            step(2 * t + 1, wide1, wide0)
        return carry
    lax.fori_loop(0, (count + 1) // 2, pair, 0)


def slot_terms(sectors, foot, own, edge):
    slots, depth, parts, lines = sectors.shape
    blocks, rows, _ = own.shape
    erows = edge.shape[1]
    quarter = lines // 4
    sectors = sectors.reshape(slots, depth, 2, 4, LANES).transpose(0, 1, 3, 2, 4).reshape(slots, depth * 8, LANES)
    hbm = pl.BlockSpec(memory_space=pltpu.HBM)
    return pl.pallas_call(
        functools.partial(slot_kernel, (slots, blocks, rows, erows)),
        in_specs=[pl.BlockSpec(memory_space=pltpu.SMEM), hbm, hbm, hbm],
        out_specs=[vmem()] * 3,
        out_shape=[jax.ShapeDtypeStruct((2, 4, r, quarter), f32) for r in (erows, rows - erows, erows)],
        scratch_shapes=[
            pltpu.VMEM((slots, depth * 8, LANES), bf16),
            pltpu.VMEM((blocks, rows, depth), bf16),
            pltpu.VMEM((blocks, erows, depth), bf16),
            pltpu.VMEM((depth * 8, LANES), f32),
            pltpu.VMEM((depth * 8, LANES), f32),
            pltpu.SemaphoreType.DMA((slots,)),
            pltpu.SemaphoreType.DMA((2,)),
        ],
        compiler_params=pltpu.CompilerParams(vmem_limit_bytes=40 << 20),
        cost_estimate=pl.CostEstimate(
            flops=4 * slots * depth * lines * (rows + erows), bytes_accessed=slots * depth * lines * 4, transcendentals=0
        ),
        name="slot_terms",
    )(foot, sectors, own, edge)


def pack_kernel(low_ref, high_ref, la, lb, ha, hb, lqa, lqb, hqa, hqb, out_ref):
    erows = low_ref.shape[2]
    for p, (lr, hr, lq, hq) in enumerate(((la, ha, lqa, hqa), (lb, hb, lqb, hqb))):
        low = low_ref[p, 3] + lr[0] + lq[...]
        out_ref[pl.ds(4 * p, LANES, stride=8), :] = low.T
        for j in range(high_ref.shape[2] // LANES):
            at = pl.ds(j * LANES, LANES)
            high = high_ref[p, 3, at] + hr[0, at] + hq[at]
            out_ref[pl.ds(4 * p + 1 + j, LANES, stride=8), :] = high.T


def pack(*args):
    return pl.pallas_call(
        pack_kernel,
        in_specs=[vmem()] * len(args),
        out_specs=vmem(),
        out_shape=jax.ShapeDtypeStruct((8 * LANES, LANES), f32),
        name="pack",
    )(*args)


def split(x):
    high = x.astype(bf16)
    return high, (x - high.astype(f32)).astype(bf16)


def tables(tiles, width):
    inner = width // LANES
    def wave(a, b, n):
        angle = 2.0 * math.pi / n * ((np.asarray(a)[:, None] * np.asarray(b)[None, :]) % n)
        return np.cos(angle), np.sin(angle)
    a = np.concatenate([2 * np.arange(tiles), 2 * np.arange(tiles) + 1])
    c, s = wave(np.arange(LANES), a, LANES)
    first = np.block([[c, -s], [s, c]])
    c, s = wave(np.arange(inner), np.arange(inner), inner)
    second = np.block([[c, -s], [s, c]])
    c, s = wave(np.arange(LANES), np.arange(inner), width)
    scale = 1.0 / math.sqrt(width)
    def halves(x):
        x = x.astype(np.float32)
        high = x.astype(jnp.bfloat16)
        return high, (x - high.astype(np.float32)).astype(jnp.bfloat16)
    return (*halves(first), *halves(second), (c * scale).astype(np.float32), (s * scale).astype(np.float32))


def image_kernel(edges, x_ref, f_hi, f_lo, s_hi, s_lo, tw_c, tw_s, out_ref, z_ref):
    tiles = x_ref.shape[0] // 16
    inner = tw_c.shape[1]

    def product(high, low, x, dims):
        xh, xl = split(x)
        dot = lambda a, b: lax.dot_general(a, b, dims, preferred_element_type=f32)
        return dot(high, xh) + dot(high, xl) + dot(low, xh)

    columns = []
    for line in range(2):
        stack = []
        for p in range(2):
            for h in range(2):
                stack.append(jnp.concatenate(
                    [x_ref[pl.ds(line * 8 + p * 4 + 2 * h + j, tiles, stride=16), :] for j in range(2)], axis=1))
        columns.append(jnp.concatenate(stack, axis=0))
    x = jnp.concatenate(columns, axis=1)
    g = product(f_hi[...], f_lo[...], x, (((1,), (0,)), ((), ())))
    rows = []
    for line in range(2):
        real = g[:LANES, line * inner:(line + 1) * inner]
        imag = g[LANES:, line * inner:(line + 1) * inner]
        c, s = tw_c[...], tw_s[...]
        rows.append(jnp.concatenate([real * c - imag * s, real * s + imag * c], axis=1))
    z_ref[...] = product(s_hi[...], s_lo[...], jnp.concatenate(rows, axis=0), (((1,), (1,)), ((), ())))

    step = 16
    chunk = step * LANES
    cell = (lax.broadcasted_iota(jnp.int32, (step, LANES), 0) * LANES
            + lax.broadcasted_iota(jnp.int32, (step, LANES), 1))

    for line in range(2):
        lower, upper = edges[line, 0], edges[line, 1]
        span = (upper - lower).astype(f32)
        at = pl.ds(line * LANES, LANES)

        def basis(i):
            n = cell + i * chunk
            inside = (n >= lower) & (n < upper)
            xi = jnp.where(inside, -1.0 + (2.0 * (n - lower).astype(f32) + 1.0) / span, 0.0)
            polys = [jnp.ones_like(xi), 4.0 * xi]
            for k in range(1, GORDER - 1):
                polys.append((2.0 * (k + 2) * xi * polys[k] - (k + 3) * polys[k - 1]) / (k + 1))
            return inside, xi, polys

        def gather(i, sums):
            inside, xi, polys = basis(i)
            base = 1.0 - xi * xi
            weight = jnp.where(inside, base * jnp.sqrt(base), 0.0)
            field = [z_ref[pl.ds(c * inner + i * step, step), at] for c in range(2)]
            out = []
            for k in range(GORDER):
                w = weight * polys[k]
                out += [sums[3 * k] + w * field[0], sums[3 * k + 1] + w * field[1], sums[3 * k + 2] + w * polys[k]]
            return tuple(out)

        begin, end = lower // chunk, (upper + chunk - 1) // chunk
        zero = jnp.zeros((step, LANES), f32)
        sums = lax.fori_loop(begin, end, gather, (zero,) * (3 * GORDER))
        total = [jnp.sum(jnp.sum(v, axis=0, keepdims=True), axis=1, keepdims=True) for v in sums]
        coef = [(total[3 * k] / total[3 * k + 2], total[3 * k + 1] / total[3 * k + 2]) for k in range(GORDER)]

        def rebuild(i, carry):
            inside, xi, polys = basis(i)
            for c in range(2):
                rebuilt = coef[0][c] * polys[0]
                for k in range(1, GORDER):
                    rebuilt = rebuilt + coef[k][c] * polys[k]
                rows = pl.ds(c * inner + i * step, step)
                z_ref[rows, at] = jnp.where(inside, rebuilt, z_ref[rows, at])
            return carry
        lax.fori_loop(begin, end, rebuild, 0)
        for c in range(2):
            out_ref[c, pl.ds(line, inner, stride=2), :] = z_ref[c * inner:(c + 1) * inner, at]


def image(edges, x, width):
    tiles = x.shape[0] // 16
    inner = width // LANES
    consts = [jnp.asarray(t) for t in tables(tiles, width)]
    out = pl.pallas_call(
        image_kernel,
        in_specs=[pl.BlockSpec(memory_space=pltpu.SMEM)] + [vmem()] * 7,
        out_specs=vmem(),
        out_shape=jax.ShapeDtypeStruct((2, 2 * inner, LANES), f32),
        scratch_shapes=[pltpu.VMEM((2 * inner, 2 * LANES), f32)],
        compiler_params=pltpu.CompilerParams(vmem_limit_bytes=24 << 20),
        name="image",
    )(edges, x, *consts)
    return out.reshape(2, inner, 2, LANES).transpose(0, 2, 1, 3).reshape(2, 2, width)


def swap(block, flip):
    return lax.ppermute(block, "aperture", [(i, i ^ flip) for i in range(4)])


def on_device(sectors, footprint, own_blocks, edge_blocks, edges):
    tiles = lax.axis_size("tile")
    low, high, rim = slot_terms(sectors[0], footprint.reshape(-1), own_blocks, edge_blocks)
    incoming = lax.ppermute(rim, "tile", [(i, i + 1) for i in range(tiles - 1)])
    ha, hb = swap(high[0, :2], 1), swap(high[1, :2], 3)
    low = low + incoming
    la, lb = swap(low[0, :2], 1), swap(low[1, :2], 3)
    hqa, hqb = swap(high[0, 2] + ha[1], 3), swap(high[1, 2] + hb[1], 1)
    lqa, lqb = swap(low[0, 2] + la[1], 3), swap(low[1, 2] + lb[1], 1)
    packed = pack(low, high, la, lb, ha, hb, lqa, lqb, hqa, hqb)
    moved = lax.all_to_all(packed.reshape(tiles, 16, LANES), "tile", 0, 0, tiled=True)
    return image(edges, moved.reshape(tiles * 16, LANES), tiles * own_blocks.shape[1])


def solution(mesh):
    in_specs = (
        P("aperture", "tile", None, None, None),
        P("aperture", "tile", None),
        P(),
        P(),
        P(("aperture", "tile"), None),
    )
    out_specs = P(None, ("aperture", "tile"), None)
    return jax.shard_map(
        on_device, mesh=mesh, in_specs=in_specs, out_specs=out_specs, check_vma=False
    )
```

```python
import functools
import math

import jax
import jax.numpy as jnp
import numpy as np
from jax import lax
from jax.experimental import pallas as pl
from jax.experimental.pallas import tpu as pltpu
from jax.sharding import PartitionSpec as P

GORDER = 8
LANES = 128
f32, bf16 = jnp.float32, jnp.bfloat16


def vmem():
    return pl.BlockSpec(memory_space=pltpu.VMEM)


def aperture(foot):
    return lax.axis_index("aperture")


def position(part, relative):
    return (relative - 1) & 3 if part == 0 else 3 - relative


def live(foot, slots, blocks):
    count = jnp.int32(0)
    for s in range(slots):
        count = count + (foot[0, s] < blocks).astype(jnp.int32)
    return count


def early_kernel(cfg, foot, x_hbm, own_hbm, edge_hbm, high_ref, rim_ref, x_ref, sums, xs, owns, edges, wide0, wide1, wide2, wide3, sems, bsem):
    slots, blocks, begin, tall, erows = cfg
    me = aperture(foot)
    depth = x_hbm.shape[1] // 8
    count = live(foot, slots, blocks)

    def fetch(s):
        return pltpu.make_async_copy(x_hbm.at[s], xs.at[s], sems.at[s])

    def start(s):
        @pl.when(s < count)
        def _():
            fetch(s).start()

    def arrive(s):
        @pl.when(s < count)
        def _():
            fetch(s).wait()

    own_copy = pltpu.make_async_copy(own_hbm.at[:, pl.ds(begin, tall), :], owns.at[pl.ds(0, blocks)], bsem.at[0])
    edge_copy = pltpu.make_async_copy(edge_hbm, edges.at[pl.ds(0, blocks)], bsem.at[1])
    fetch(0).start()
    start(1)
    own_copy.start()
    edge_copy.start()
    for s in range(2, slots):
        start(s)
    owns[blocks] = jnp.zeros((tall, depth), bf16)
    edges[blocks] = jnp.zeros((erows, depth), bf16)
    sums[...] = jnp.zeros_like(sums)

    def widen(s, wide):
        wide[...] = xs[jnp.minimum(s, count - 1)].astype(f32)

    def kernels(s):
        at = jnp.minimum(s, count - 1)
        o, e = foot[0, at], foot[1, at]
        own = owns[jnp.where(s < count, o, blocks)]
        edge = edges[jnp.where(s < count, e, blocks)]
        return jnp.concatenate([own, edge], axis=0)

    def columns(p, wide):
        return jnp.concatenate([wide[pl.ds(2 * j + p, depth, stride=8), :].astype(bf16) for j in range(4)], axis=1)

    def multiply(s, first, second):
        ka, kb = kernels(s), kernels(s + 1)
        for p in range(2):
            xa, xb = columns(p, first), columns(p, second)
            x_ref[s, p] = xa
            x_ref[s + 1, p] = xb
            y = jnp.dot(ka, xa, preferred_element_type=f32) + jnp.dot(kb, xb, preferred_element_type=f32)
            sums[p] += y

    fetch(0).wait()
    widen(0, wide0)
    arrive(1)
    widen(1, wide1)
    own_copy.wait()
    edge_copy.wait()

    def step(s, here, there):
        arrive(s + 2)
        arrive(s + 3)
        widen(s + 2, there[0])
        widen(s + 3, there[1])
        multiply(s, *here)

    def quad(t, carry):
        step(4 * t, (wide0, wide1), (wide2, wide3))

        @pl.when(4 * t + 2 < count)
        def _():
            step(4 * t + 2, (wide2, wide3), (wide0, wide1))
        return carry
    lax.fori_loop(0, (count + 3) // 4, quad, 0)
    for p in range(2):
        for j in range(4):
            pos = position(p, me ^ j)
            high_ref[p, pos] = sums[p, :tall, j * LANES:(j + 1) * LANES]
            rim_ref[p, pos] = sums[p, tall:, j * LANES:(j + 1) * LANES]


def early_terms(sectors, foot, own, edge, begin):
    slots, depth, parts, lines = sectors.shape
    blocks, rows, _ = own.shape
    tall, erows = rows - begin, edge.shape[1]
    quarter = lines // 4
    sectors = sectors.reshape(slots, depth, 2, 4, LANES).transpose(0, 1, 3, 2, 4).reshape(slots, depth * 8, LANES)
    hbm = pl.BlockSpec(memory_space=pltpu.HBM)
    return pl.pallas_call(
        functools.partial(early_kernel, (slots, blocks, begin, tall, erows)),
        in_specs=[pl.BlockSpec(memory_space=pltpu.SMEM), hbm, hbm, hbm],
        out_specs=[vmem()] * 3,
        out_shape=[jax.ShapeDtypeStruct((2, 4, r, quarter), f32) for r in (tall, erows)]
        + [jax.ShapeDtypeStruct((slots, 2, depth, lines), bf16)],
        scratch_shapes=[
            pltpu.VMEM((2, tall + erows, lines), f32),
            pltpu.VMEM((slots, depth * 8, LANES), bf16),
            pltpu.VMEM((blocks + 1, tall, depth), bf16),
            pltpu.VMEM((blocks + 1, erows, depth), bf16),
            *[pltpu.VMEM((depth * 8, LANES), f32)] * 4,
            pltpu.SemaphoreType.DMA((slots,)),
            pltpu.SemaphoreType.DMA((2,)),
        ],
        compiler_params=pltpu.CompilerParams(vmem_limit_bytes=36 << 20),
        cost_estimate=pl.CostEstimate(
            flops=4 * slots * depth * lines * (tall + erows), bytes_accessed=slots * depth * lines * 4, transcendentals=0
        ),
        name="early_terms",
    )(foot, *[pltpu.with_memory_space_constraint(v, pltpu.HBM) for v in (sectors, own, edge)])


def late_kernel(cfg, foot, x_ref, own_ref, low_ref, sums):
    slots, blocks, tall = cfg
    me = aperture(foot)
    count = live(foot, slots, blocks)
    sums[...] = jnp.zeros_like(sums)

    def add(s, ops):
        for p in range(2):
            y = sum(jnp.dot(own_ref[foot[0, s + i], :tall], x_ref[s + i, p], preferred_element_type=f32) for i in ops)
            sums[p] += y

    def pair(t, carry):
        add(2 * t, (0, 1))
        return carry
    lax.fori_loop(0, count // 2, pair, 0)

    @pl.when(count % 2 == 1)
    def _():
        add(count - 1, (0,))
    for p in range(2):
        for j in range(4):
            low_ref[p, position(p, me ^ j)] = sums[p, :, j * LANES:(j + 1) * LANES]


def late_terms(x, foot, own, tall):
    slots, parts, depth, lines = x.shape
    blocks = own.shape[0]
    return pl.pallas_call(
        functools.partial(late_kernel, (slots, blocks, tall)),
        in_specs=[pl.BlockSpec(memory_space=pltpu.SMEM), vmem(), vmem()],
        out_specs=vmem(),
        out_shape=jax.ShapeDtypeStruct((2, 4, tall, lines // 4), f32),
        scratch_shapes=[pltpu.VMEM((2, tall, lines), f32)],
        compiler_params=pltpu.CompilerParams(vmem_limit_bytes=24 << 20),
        cost_estimate=pl.CostEstimate(
            flops=4 * slots * depth * lines * tall, bytes_accessed=slots * depth * lines * 4, transcendentals=0
        ),
        name="late_terms",
    )(foot, x, own)


def pack_kernel(*refs):
    *terms, out_ref = refs
    for p in range(2):
        keeps, firsts, second = terms[5 * p:5 * p + 2], terms[5 * p + 2:5 * p + 4], terms[5 * p + 4]
        row = 0
        for keep, first in zip(keeps, firsts):
            for j in range(keep.shape[0] // LANES):
                at = pl.ds(j * LANES, LANES)
                total = keep[at] + first[at] + second[pl.ds(row * LANES, LANES)]
                out_ref[pl.ds(4 * p + row, LANES, stride=8), :] = total.T
                row += 1


def pack(*args):
    return pl.pallas_call(
        pack_kernel,
        in_specs=[vmem()] * len(args),
        out_specs=vmem(),
        out_shape=jax.ShapeDtypeStruct((8 * LANES, LANES), f32),
        compiler_params=pltpu.CompilerParams(vmem_limit_bytes=8 << 20),
        name="pack",
    )(*args)


def split(x):
    high = x.astype(bf16)
    return high, (x - high.astype(f32)).astype(bf16)


def tables(tiles, width):
    inner = width // LANES
    def wave(a, b, n):
        angle = 2.0 * math.pi / n * ((np.asarray(a)[:, None] * np.asarray(b)[None, :]) % n)
        return np.cos(angle), np.sin(angle)
    a = np.concatenate([2 * np.arange(tiles), 2 * np.arange(tiles) + 1])
    c, s = wave(np.arange(LANES), a, LANES)
    first = np.block([[c, -s], [s, c]])
    c, s = wave(np.arange(inner), np.arange(inner), inner)
    second = np.block([[c, -s], [s, c]])
    c, s = wave(np.arange(LANES), np.arange(inner), width)
    scale = 1.0 / math.sqrt(width)
    def halves(x):
        x = x.astype(np.float32)
        high = x.astype(jnp.bfloat16)
        return high, (x - high.astype(np.float32)).astype(jnp.bfloat16)
    return (*halves(first), *halves(second), (c * scale).astype(np.float32), (s * scale).astype(np.float32))


def image_kernel(edges, x_ref, f_hi, f_lo, s_hi, s_lo, tw_c, tw_s, out_ref, z_ref):
    tiles = x_ref.shape[0] // 16
    inner = tw_c.shape[1]

    def product(high, low, x, dims):
        xh, xl = split(x)
        dot = lambda a, b: lax.dot_general(a, b, dims, preferred_element_type=f32)
        return dot(high, xh) + dot(high, xl) + dot(low, xh)

    columns = []
    for line in range(2):
        stack = []
        for p in range(2):
            for h in range(2):
                stack.append(jnp.concatenate(
                    [x_ref[pl.ds(line * 8 + p * 4 + 2 * h + j, tiles, stride=16), :] for j in range(2)], axis=1))
        columns.append(jnp.concatenate(stack, axis=0))
    x = jnp.concatenate(columns, axis=1)
    g = product(f_hi[...], f_lo[...], x, (((1,), (0,)), ((), ())))
    rows = []
    for line in range(2):
        real = g[:LANES, line * inner:(line + 1) * inner]
        imag = g[LANES:, line * inner:(line + 1) * inner]
        c, s = tw_c[...], tw_s[...]
        rows.append(jnp.concatenate([real * c - imag * s, real * s + imag * c], axis=1))
    z_ref[...] = product(s_hi[...], s_lo[...], jnp.concatenate(rows, axis=0), (((1,), (1,)), ((), ())))

    step = 16
    chunk = step * LANES
    cell = (lax.broadcasted_iota(jnp.int32, (step, LANES), 0) * LANES
            + lax.broadcasted_iota(jnp.int32, (step, LANES), 1))

    for line in range(2):
        lower, upper = edges[line, 0], edges[line, 1]
        span = (upper - lower).astype(f32)
        at = pl.ds(line * LANES, LANES)

        def basis(i):
            n = cell + i * chunk
            inside = (n >= lower) & (n < upper)
            xi = jnp.where(inside, -1.0 + (2.0 * (n - lower).astype(f32) + 1.0) / span, 0.0)
            polys = [jnp.ones_like(xi), 4.0 * xi]
            for k in range(1, GORDER - 1):
                polys.append((2.0 * (k + 2) * xi * polys[k] - (k + 3) * polys[k - 1]) / (k + 1))
            return inside, xi, polys

        def gather(i, sums):
            inside, xi, polys = basis(i)
            base = 1.0 - xi * xi
            weight = jnp.where(inside, base * jnp.sqrt(base), 0.0)
            field = [z_ref[pl.ds(c * inner + i * step, step), at] for c in range(2)]
            out = []
            for k in range(GORDER):
                w = weight * polys[k]
                out += [sums[3 * k] + w * field[0], sums[3 * k + 1] + w * field[1], sums[3 * k + 2] + w * polys[k]]
            return tuple(out)

        begin, end = lower // chunk, (upper + chunk - 1) // chunk
        zero = jnp.zeros((step, LANES), f32)
        sums = lax.fori_loop(begin, end, gather, (zero,) * (3 * GORDER))
        total = [jnp.sum(jnp.sum(v, axis=0, keepdims=True), axis=1, keepdims=True) for v in sums]
        coef = [(total[3 * k] / total[3 * k + 2], total[3 * k + 1] / total[3 * k + 2]) for k in range(GORDER)]

        def rebuild(i, carry):
            inside, xi, polys = basis(i)
            for c in range(2):
                rebuilt = coef[0][c] * polys[0]
                for k in range(1, GORDER):
                    rebuilt = rebuilt + coef[k][c] * polys[k]
                rows = pl.ds(c * inner + i * step, step)
                z_ref[rows, at] = jnp.where(inside, rebuilt, z_ref[rows, at])
            return carry
        lax.fori_loop(begin, end, rebuild, 0)
        for c in range(2):
            out_ref[c, pl.ds(line, inner, stride=2), :] = z_ref[c * inner:(c + 1) * inner, at]


def image(edges, x, width):
    tiles = x.shape[0] // 16
    inner = width // LANES
    consts = [jnp.asarray(t) for t in tables(tiles, width)]
    out = pl.pallas_call(
        image_kernel,
        in_specs=[pl.BlockSpec(memory_space=pltpu.SMEM)] + [vmem()] * 7,
        out_specs=vmem(),
        out_shape=jax.ShapeDtypeStruct((2, 2 * inner, LANES), f32),
        scratch_shapes=[pltpu.VMEM((2 * inner, 2 * LANES), f32)],
        compiler_params=pltpu.CompilerParams(vmem_limit_bytes=12 << 20),
        name="image",
    )(edges, x, *consts)
    return out.reshape(2, inner, 2, LANES).transpose(0, 2, 1, 3).reshape(2, 2, width)


def swap(block, flip):
    return lax.ppermute(block, "aperture", [(i, i ^ flip) for i in range(4)])


def on_device(sectors, footprint, own_blocks, edge_blocks, edges):
    tiles = lax.axis_size("tile")
    foot = footprint[0].T
    half = own_blocks.shape[1] // 2
    high, rim, spread = early_terms(sectors[0], foot, own_blocks, edge_blocks, half)
    incoming = lax.ppermute(rim, "tile", [(i, i + 1) for i in range(tiles - 1)])
    ha, hb = swap(high[0, :2], 1), swap(high[1, :2], 3)
    low = late_terms(spread, foot, own_blocks, half)
    low = low + jnp.pad(incoming, ((0, 0), (0, 0), (0, half - incoming.shape[2]), (0, 0)))
    la, lb = swap(low[0, :2], 1), swap(low[1, :2], 3)
    qa = swap(jnp.concatenate([low[0, 2] + la[1], high[0, 2] + ha[1]]), 3)
    qb = swap(jnp.concatenate([low[1, 2] + lb[1], high[1, 2] + hb[1]]), 1)
    packed = pack(low[0, 3], high[0, 3], la[0], ha[0], qa, low[1, 3], high[1, 3], lb[0], hb[0], qb)
    moved = lax.all_to_all(packed.reshape(tiles, 16, LANES), "tile", 0, 0, tiled=True)
    return image(edges, moved.reshape(tiles * 16, LANES), tiles * own_blocks.shape[1])


def solution(mesh):
    in_specs = (
        P("aperture", "tile", None, None, None),
        P("aperture", "tile", None),
        P(),
        P(),
        P(("aperture", "tile"), None),
    )
    out_specs = P(None, ("aperture", "tile"), None)
    return jax.shard_map(
        on_device, mesh=mesh, in_specs=in_specs, out_specs=out_specs, check_vma=False
    )
```

```python
import functools
import math

import jax
import jax.numpy as jnp
import numpy as np
from jax import lax
from jax.experimental import pallas as pl
from jax.experimental.pallas import tpu as pltpu
from jax.sharding import PartitionSpec as P

GORDER = 8
LANES = 128
f32, bf16 = jnp.float32, jnp.bfloat16


def vmem():
    return pl.BlockSpec(memory_space=pltpu.VMEM)


def aperture(foot):
    return lax.axis_index("aperture")


def live(foot, slots, blocks):
    count = jnp.int32(0)
    for s in range(slots):
        count = count + (foot[0, s] < blocks).astype(jnp.int32)
    return count


def early_kernel(cfg, foot, x_hbm, own_hbm, edge_hbm, high_ref, rim_ref, x_ref, sums, xs, owns, edges, wide0, wide1, wide2, wide3, sems, bsem):
    slots, blocks, begin, tall, erows = cfg
    me = aperture(foot)
    depth = x_hbm.shape[1] // 8
    count = live(foot, slots, blocks)

    def fetch(s):
        return pltpu.make_async_copy(x_hbm.at[s], xs.at[s], sems.at[s])

    def start(s):
        @pl.when(s < count)
        def _():
            fetch(s).start()

    def arrive(s):
        @pl.when(s < count)
        def _():
            fetch(s).wait()

    own_copy = pltpu.make_async_copy(own_hbm.at[:, pl.ds(begin, tall), :], owns.at[pl.ds(0, blocks)], bsem.at[0])
    edge_copy = pltpu.make_async_copy(edge_hbm, edges.at[pl.ds(0, blocks)], bsem.at[1])
    fetch(0).start()
    start(1)
    own_copy.start()
    edge_copy.start()
    for s in range(2, 4):
        start(s)
    owns[blocks] = jnp.zeros((tall, depth), bf16)
    edges[blocks] = jnp.zeros((erows, depth), bf16)
    sums[...] = jnp.zeros_like(sums)

    def widen(s, wide):
        wide[...] = xs[jnp.minimum(s, count - 1)].astype(f32)

    def kernels(s):
        at = jnp.minimum(s, count - 1)
        o, e = foot[0, at], foot[1, at]
        own = owns[jnp.where(s < count, o, blocks)]
        edge = edges[jnp.where(s < count, e, blocks)]
        return jnp.concatenate([own, edge], axis=0)

    def columns(p, wide):
        return jnp.concatenate([wide[pl.ds(2 * j + p, depth, stride=8), :].astype(bf16) for j in range(4)], axis=1)

    def multiply(s, first, second):
        ka, kb = kernels(s), kernels(s + 1)
        for p in range(2):
            xa, xb = columns(p, first), columns(p, second)
            x_ref[s, p] = xa
            x_ref[s + 1, p] = xb
            y = jnp.dot(ka, xa, preferred_element_type=f32) + jnp.dot(kb, xb, preferred_element_type=f32)
            sums[p] += y

    fetch(0).wait()
    widen(0, wide0)
    arrive(1)
    widen(1, wide1)
    own_copy.wait()
    edge_copy.wait()
    for s in range(4, slots):
        start(s)

    def step(s, here, there):
        arrive(s + 2)
        arrive(s + 3)
        widen(s + 2, there[0])
        widen(s + 3, there[1])
        multiply(s, *here)

    def quad(t, carry):
        step(4 * t, (wide0, wide1), (wide2, wide3))

        @pl.when(4 * t + 2 < count)
        def _():
            step(4 * t + 2, (wide2, wide3), (wide0, wide1))
        return carry
    lax.fori_loop(0, (count + 3) // 4, quad, 0)
    for p in range(2):
        for j in range(4):
            high_ref[me ^ j, p] = sums[p, :tall, j * LANES:(j + 1) * LANES]
            rim_ref[me ^ j, p] = sums[p, tall:, j * LANES:(j + 1) * LANES]


def early_terms(sectors, foot, own, edge, begin):
    slots, depth, parts, lines = sectors.shape
    blocks, rows, _ = own.shape
    tall, erows = rows - begin, edge.shape[1]
    quarter = lines // 4
    sectors = sectors.reshape(slots, depth, 2, 4, LANES).transpose(0, 1, 3, 2, 4).reshape(slots, depth * 8, LANES)
    hbm = pl.BlockSpec(memory_space=pltpu.HBM)
    return pl.pallas_call(
        functools.partial(early_kernel, (slots, blocks, begin, tall, erows)),
        in_specs=[pl.BlockSpec(memory_space=pltpu.SMEM), hbm, hbm, hbm],
        out_specs=[vmem()] * 3,
        out_shape=[jax.ShapeDtypeStruct((4, 2, r, quarter), f32) for r in (tall, erows)]
        + [jax.ShapeDtypeStruct((slots, 2, depth, lines), bf16)],
        scratch_shapes=[
            pltpu.VMEM((2, tall + erows, lines), f32),
            pltpu.VMEM((slots, depth * 8, LANES), bf16),
            pltpu.VMEM((blocks + 1, tall, depth), bf16),
            pltpu.VMEM((blocks + 1, erows, depth), bf16),
            *[pltpu.VMEM((depth * 8, LANES), f32)] * 4,
            pltpu.SemaphoreType.DMA((slots,)),
            pltpu.SemaphoreType.DMA((2,)),
        ],
        compiler_params=pltpu.CompilerParams(vmem_limit_bytes=36 << 20),
        cost_estimate=pl.CostEstimate(
            flops=4 * slots * depth * lines * (tall + erows), bytes_accessed=slots * depth * lines * 4, transcendentals=0
        ),
        name="early_terms",
    )(pltpu.with_memory_space_constraint(foot, pltpu.HBM), *[pltpu.with_memory_space_constraint(v, pltpu.HBM) for v in (sectors, own, edge)])


def late_kernel(cfg, foot, x_ref, own_ref, low_ref, sums):
    slots, blocks, tall = cfg
    me = aperture(foot)
    count = live(foot, slots, blocks)
    sums[...] = jnp.zeros_like(sums)

    def add(s, ops):
        for p in range(2):
            y = sum(jnp.dot(own_ref[foot[0, s + i], :tall], x_ref[s + i, p], preferred_element_type=f32) for i in ops)
            sums[p] += y

    def pair(t, carry):
        add(2 * t, (0, 1))
        return carry
    lax.fori_loop(0, count // 2, pair, 0)

    @pl.when(count % 2 == 1)
    def _():
        add(count - 1, (0,))
    for p in range(2):
        for j in range(4):
            low_ref[me ^ j, p] = sums[p, :, j * LANES:(j + 1) * LANES]


def late_terms(x, foot, own, tall):
    slots, parts, depth, lines = x.shape
    blocks = own.shape[0]
    return pl.pallas_call(
        functools.partial(late_kernel, (slots, blocks, tall)),
        in_specs=[pl.BlockSpec(memory_space=pltpu.SMEM), vmem(), vmem()],
        out_specs=vmem(),
        out_shape=jax.ShapeDtypeStruct((4, 2, tall, lines // 4), f32),
        scratch_shapes=[pltpu.VMEM((2, tall, lines), f32)],
        compiler_params=pltpu.CompilerParams(vmem_limit_bytes=24 << 20),
        cost_estimate=pl.CostEstimate(
            flops=4 * slots * depth * lines * tall, bytes_accessed=slots * depth * lines * 4, transcendentals=0
        ),
        name="late_terms",
    )(pltpu.with_memory_space_constraint(foot, pltpu.HBM), x, own)


def pack_kernel(lows, *refs):
    *terms, out_ref = refs
    for p in range(2):
        row = 4 * p
        for group in (terms[:lows], terms[lows:]):
            for j in range(group[0].shape[1] // LANES):
                at = pl.ds(j * LANES, LANES)
                out_ref[pl.ds(row, LANES, stride=8), :] = sum(term[p, at] for term in group).T
                row += 1


def pack(low, high):
    return pl.pallas_call(
        functools.partial(pack_kernel, len(low)),
        in_specs=[vmem()] * (len(low) + len(high)),
        out_specs=vmem(),
        out_shape=jax.ShapeDtypeStruct((8 * LANES, LANES), f32),
        compiler_params=pltpu.CompilerParams(vmem_limit_bytes=8 << 20),
        name="pack",
    )(*low, *high)


def split(x):
    high = x.astype(bf16)
    return high, (x - high.astype(f32)).astype(bf16)


def tables(tiles, width):
    inner = width // LANES
    def wave(a, b, n):
        angle = 2.0 * math.pi / n * ((np.asarray(a)[:, None] * np.asarray(b)[None, :]) % n)
        return np.cos(angle), np.sin(angle)
    a = np.concatenate([2 * np.arange(tiles), 2 * np.arange(tiles) + 1])
    c, s = wave(np.arange(LANES), a, LANES)
    first = np.block([[c, -s], [s, c]])
    c, s = wave(np.arange(inner), np.arange(inner), inner)
    second = np.block([[c, -s], [s, c]])
    c, s = wave(np.arange(LANES), np.arange(inner), width)
    scale = 1.0 / math.sqrt(width)
    def halves(x):
        x = x.astype(np.float32)
        high = x.astype(jnp.bfloat16)
        return high, (x - high.astype(np.float32)).astype(jnp.bfloat16)
    return (*halves(first), *halves(second), (c * scale).astype(np.float32), (s * scale).astype(np.float32))


def image_kernel(edges, x_ref, f_hi, f_lo, s_hi, s_lo, tw_c, tw_s, out_ref, z_ref):
    tiles = x_ref.shape[0] // 16
    inner = tw_c.shape[1]

    def product(high, low, x, dims):
        xh, xl = split(x)
        dot = lambda a, b: lax.dot_general(a, b, dims, preferred_element_type=f32)
        return dot(high, xh) + dot(high, xl) + dot(low, xh)

    columns = []
    for line in range(2):
        stack = []
        for p in range(2):
            for h in range(2):
                stack.append(jnp.concatenate(
                    [x_ref[pl.ds(line * 8 + p * 4 + 2 * h + j, tiles, stride=16), :] for j in range(2)], axis=1))
        columns.append(jnp.concatenate(stack, axis=0))
    x = jnp.concatenate(columns, axis=1)
    g = product(f_hi[...], f_lo[...], x, (((1,), (0,)), ((), ())))
    rows = []
    for line in range(2):
        real = g[:LANES, line * inner:(line + 1) * inner]
        imag = g[LANES:, line * inner:(line + 1) * inner]
        c, s = tw_c[...], tw_s[...]
        rows.append(jnp.concatenate([real * c - imag * s, real * s + imag * c], axis=1))
    z_ref[...] = product(s_hi[...], s_lo[...], jnp.concatenate(rows, axis=0), (((1,), (1,)), ((), ())))

    step = 16
    chunk = step * LANES
    cell = (lax.broadcasted_iota(jnp.int32, (step, LANES), 0) * LANES
            + lax.broadcasted_iota(jnp.int32, (step, LANES), 1))

    for line in range(2):
        lower, upper = edges[line, 0], edges[line, 1]
        span = (upper - lower).astype(f32)
        at = pl.ds(line * LANES, LANES)

        def basis(i):
            n = cell + i * chunk
            inside = (n >= lower) & (n < upper)
            xi = jnp.where(inside, -1.0 + (2.0 * (n - lower).astype(f32) + 1.0) / span, 0.0)
            polys = [jnp.ones_like(xi), 4.0 * xi]
            for k in range(1, GORDER - 1):
                polys.append((2.0 * (k + 2) * xi * polys[k] - (k + 3) * polys[k - 1]) / (k + 1))
            return inside, xi, polys

        def gather(i, sums):
            inside, xi, polys = basis(i)
            base = 1.0 - xi * xi
            weight = jnp.where(inside, base * jnp.sqrt(base), 0.0)
            field = [z_ref[pl.ds(c * inner + i * step, step), at] for c in range(2)]
            out = []
            for k in range(GORDER):
                w = weight * polys[k]
                out += [sums[3 * k] + w * field[0], sums[3 * k + 1] + w * field[1], sums[3 * k + 2] + w * polys[k]]
            return tuple(out)

        begin, end = lower // chunk, (upper + chunk - 1) // chunk
        zero = jnp.zeros((step, LANES), f32)
        sums = lax.fori_loop(begin, end, gather, (zero,) * (3 * GORDER))
        total = [jnp.sum(jnp.sum(v, axis=0, keepdims=True), axis=1, keepdims=True) for v in sums]
        coef = [(total[3 * k] / total[3 * k + 2], total[3 * k + 1] / total[3 * k + 2]) for k in range(GORDER)]

        def rebuild(i, carry):
            inside, xi, polys = basis(i)
            for c in range(2):
                rebuilt = coef[0][c] * polys[0]
                for k in range(1, GORDER):
                    rebuilt = rebuilt + coef[k][c] * polys[k]
                rows = pl.ds(c * inner + i * step, step)
                z_ref[rows, at] = jnp.where(inside, rebuilt, z_ref[rows, at])
            return carry
        lax.fori_loop(begin, end, rebuild, 0)
        for c in range(2):
            out_ref[c, pl.ds(line, inner, stride=2), :] = z_ref[c * inner:(c + 1) * inner, at]


def image(edges, x, width):
    tiles = x.shape[0] // 16
    inner = width // LANES
    consts = [jnp.asarray(t) for t in tables(tiles, width)]
    out = pl.pallas_call(
        image_kernel,
        in_specs=[pl.BlockSpec(memory_space=pltpu.SMEM)] + [vmem()] * 7,
        out_specs=vmem(),
        out_shape=jax.ShapeDtypeStruct((2, 2 * inner, LANES), f32),
        scratch_shapes=[pltpu.VMEM((2 * inner, 2 * LANES), f32)],
        compiler_params=pltpu.CompilerParams(vmem_limit_bytes=12 << 20),
        name="image",
    )(edges, x, *consts)
    return out.reshape(2, inner, 2, LANES).transpose(0, 2, 1, 3).reshape(2, 2, width)


def swap(block, flip):
    return lax.ppermute(block, "aperture", [(i, i ^ flip) for i in range(4)])


def on_device(sectors, footprint, own_blocks, edge_blocks, edges):
    tiles = lax.axis_size("tile")
    foot = footprint[0].T
    half = own_blocks.shape[1] // 2
    high, rim, spread = early_terms(sectors[0], foot, own_blocks, edge_blocks, half)
    incoming = lax.ppermute(rim, "tile", [(i, i + 1) for i in range(tiles - 1)])
    highs = [high[0]] + [swap(high[r], r) for r in (1, 3, 2)]
    low = late_terms(spread, foot, own_blocks, half)
    low = low + jnp.pad(incoming, ((0, 0), (0, 0), (0, half - incoming.shape[2]), (0, 0)))
    lows = [low[0]] + [swap(low[r], r) for r in (1, 3, 2)]
    packed = pack(lows, highs)
    moved = lax.all_to_all(packed.reshape(tiles, 16, LANES), "tile", 0, 0, tiled=True)
    return image(edges, moved.reshape(tiles * 16, LANES), tiles * own_blocks.shape[1])


def solution(mesh):
    in_specs = (
        P("aperture", "tile", None, None, None),
        P("aperture", "tile", None),
        P(),
        P(),
        P(("aperture", "tile"), None),
    )
    out_specs = P(None, ("aperture", "tile"), None)
    return jax.shard_map(
        on_device, mesh=mesh, in_specs=in_specs, out_specs=out_specs, check_vma=False
    )
```

```python
import functools
import math

import jax
import jax.numpy as jnp
import numpy as np
from jax import lax
from jax.experimental import pallas as pl
from jax.experimental.pallas import tpu as pltpu
from jax.sharding import PartitionSpec as P

GORDER = 8
LANES = 128
f32, bf16 = jnp.float32, jnp.bfloat16


def vmem():
    return pl.BlockSpec(memory_space=pltpu.VMEM)


def aperture(foot):
    return lax.axis_index("aperture")


def live(foot, slots, blocks):
    count = jnp.int32(0)
    for s in range(slots):
        count = count + (foot[0, s] < blocks).astype(jnp.int32)
    return count


def early_kernel(cfg, foot, x_hbm, own_hbm, edge_hbm, high_ref, rim_ref, x_ref, sums, xs, owns, edges, wide0, wide1, wide2, wide3, sems, bsem):
    slots, blocks, begin, tall, erows = cfg
    me = aperture(foot)
    depth = x_hbm.shape[1] // 8
    count = live(foot, slots, blocks)

    def fetch(s):
        return pltpu.make_async_copy(x_hbm.at[s], xs.at[s], sems.at[s])

    def start(s):
        @pl.when(s < count)
        def _():
            fetch(s).start()

    def arrive(s):
        @pl.when(s < count)
        def _():
            fetch(s).wait()

    own_copy = pltpu.make_async_copy(own_hbm.at[:, pl.ds(begin, tall), :], owns.at[pl.ds(0, blocks)], bsem.at[0])
    edge_copy = pltpu.make_async_copy(edge_hbm, edges.at[pl.ds(0, blocks)], bsem.at[1])
    fetch(0).start()
    start(1)
    own_copy.start()
    edge_copy.start()
    for s in range(2, 4):
        start(s)
    owns[blocks] = jnp.zeros((tall, depth), bf16)
    edges[blocks] = jnp.zeros((erows, depth), bf16)
    sums[...] = jnp.zeros_like(sums)

    def widen(s, wide):
        wide[...] = xs[jnp.minimum(s, count - 1)].astype(f32)

    def kernels(s):
        at = jnp.minimum(s, count - 1)
        o, e = foot[0, at], foot[1, at]
        own = owns[jnp.where(s < count, o, blocks)]
        edge = edges[jnp.where(s < count, e, blocks)]
        return jnp.concatenate([own, edge], axis=0)

    def columns(p, wide):
        return jnp.concatenate([wide[pl.ds(2 * j + p, depth, stride=8), :].astype(bf16) for j in range(4)], axis=1)

    def multiply(s, first, second):
        ka, kb = kernels(s), kernels(s + 1)
        for p in range(2):
            xa, xb = columns(p, first), columns(p, second)
            x_ref[s, p] = xa
            x_ref[s + 1, p] = xb
            y = jnp.dot(ka, xa, preferred_element_type=f32) + jnp.dot(kb, xb, preferred_element_type=f32)
            sums[p] += y

    fetch(0).wait()
    widen(0, wide0)
    arrive(1)
    widen(1, wide1)
    own_copy.wait()
    edge_copy.wait()
    for s in range(4, slots):
        start(s)

    def step(s, here, there):
        arrive(s + 2)
        arrive(s + 3)
        widen(s + 2, there[0])
        widen(s + 3, there[1])
        multiply(s, *here)

    def quad(t, carry):
        step(4 * t, (wide0, wide1), (wide2, wide3))

        @pl.when(4 * t + 2 < count)
        def _():
            step(4 * t + 2, (wide2, wide3), (wide0, wide1))
        return carry
    lax.fori_loop(0, (count + 3) // 4, quad, 0)
    for p in range(2):
        for j in range(4):
            high_ref[me ^ j, p] = sums[p, :tall, j * LANES:(j + 1) * LANES]
            rim_ref[me ^ j, p] = sums[p, tall:, j * LANES:(j + 1) * LANES]


def early_terms(sectors, foot, own, edge, begin):
    slots, depth, parts, lines = sectors.shape
    blocks, rows, _ = own.shape
    tall, erows = rows - begin, edge.shape[1]
    quarter = lines // 4
    sectors = sectors.reshape(slots, depth, 2, 4, LANES).transpose(0, 1, 3, 2, 4).reshape(slots, depth * 8, LANES)
    hbm = pl.BlockSpec(memory_space=pltpu.HBM)
    return pl.pallas_call(
        functools.partial(early_kernel, (slots, blocks, begin, tall, erows)),
        in_specs=[pl.BlockSpec(memory_space=pltpu.SMEM), hbm, hbm, hbm],
        out_specs=[vmem()] * 3,
        out_shape=[jax.ShapeDtypeStruct((4, 2, r, quarter), f32) for r in (tall, erows)]
        + [jax.ShapeDtypeStruct((slots, 2, depth, lines), bf16)],
        scratch_shapes=[
            pltpu.VMEM((2, tall + erows, lines), f32),
            pltpu.VMEM((slots, depth * 8, LANES), bf16),
            pltpu.VMEM((blocks + 1, tall, depth), bf16),
            pltpu.VMEM((blocks + 1, erows, depth), bf16),
            *[pltpu.VMEM((depth * 8, LANES), f32)] * 4,
            pltpu.SemaphoreType.DMA((slots,)),
            pltpu.SemaphoreType.DMA((2,)),
        ],
        compiler_params=pltpu.CompilerParams(vmem_limit_bytes=38 << 20),
        cost_estimate=pl.CostEstimate(
            flops=4 * slots * depth * lines * (tall + erows), bytes_accessed=slots * depth * lines * 4, transcendentals=0
        ),
        name="early_terms",
    )(pltpu.with_memory_space_constraint(foot, pltpu.HBM), *[pltpu.with_memory_space_constraint(v, pltpu.HBM) for v in (sectors, own, edge)])


def late_kernel(cfg, foot, x_ref, own_ref, low_ref, sums):
    slots, blocks, tall = cfg
    me = aperture(foot)
    count = live(foot, slots, blocks)
    sums[...] = jnp.zeros_like(sums)

    def add(s, ops):
        for p in range(2):
            y = sum(jnp.dot(own_ref[foot[0, s + i], :tall], x_ref[s + i, p], preferred_element_type=f32) for i in ops)
            sums[p] += y

    def pair(t, carry):
        add(2 * t, (0, 1))
        return carry
    lax.fori_loop(0, count // 2, pair, 0)

    @pl.when(count % 2 == 1)
    def _():
        add(count - 1, (0,))
    for p in range(2):
        for j in range(4):
            low_ref[me ^ j, p] = sums[p, :, j * LANES:(j + 1) * LANES]


def late_terms(x, foot, own, tall):
    slots, parts, depth, lines = x.shape
    blocks = own.shape[0]
    return pl.pallas_call(
        functools.partial(late_kernel, (slots, blocks, tall)),
        in_specs=[pl.BlockSpec(memory_space=pltpu.SMEM), vmem(), vmem()],
        out_specs=vmem(),
        out_shape=jax.ShapeDtypeStruct((4, 2, tall, lines // 4), f32),
        scratch_shapes=[pltpu.VMEM((2, tall, lines), f32)],
        compiler_params=pltpu.CompilerParams(vmem_limit_bytes=24 << 20),
        cost_estimate=pl.CostEstimate(
            flops=4 * slots * depth * lines * tall, bytes_accessed=slots * depth * lines * 4, transcendentals=0
        ),
        name="late_terms",
    )(pltpu.with_memory_space_constraint(foot, pltpu.HBM), x, own)


def pack_kernel(lows, *refs):
    *terms, out_ref = refs
    for p in range(2):
        row = 4 * p
        for group in (terms[:lows], terms[lows:]):
            for j in range(group[0].shape[1] // LANES):
                at = pl.ds(j * LANES, LANES)
                out_ref[pl.ds(row, LANES, stride=8), :] = sum(term[p, at] for term in group).T
                row += 1


def pack(low, high):
    return pl.pallas_call(
        functools.partial(pack_kernel, len(low)),
        in_specs=[vmem()] * (len(low) + len(high)),
        out_specs=vmem(),
        out_shape=jax.ShapeDtypeStruct((8 * LANES, LANES), f32),
        compiler_params=pltpu.CompilerParams(vmem_limit_bytes=8 << 20),
        name="pack",
    )(*low, *high)


def split(x):
    high = x.astype(bf16)
    return high, (x - high.astype(f32)).astype(bf16)


def tables(tiles, width):
    inner = width // LANES
    def wave(a, b, n):
        angle = 2.0 * math.pi / n * ((np.asarray(a)[:, None] * np.asarray(b)[None, :]) % n)
        return np.cos(angle), np.sin(angle)
    a = np.concatenate([2 * np.arange(tiles), 2 * np.arange(tiles) + 1])
    c, s = wave(np.arange(LANES), a, LANES)
    first = np.block([[c, -s], [s, c]])
    c, s = wave(np.arange(inner), np.arange(inner), inner)
    second = np.block([[c, -s], [s, c]])
    c, s = wave(np.arange(LANES), np.arange(inner), width)
    scale = 1.0 / math.sqrt(width)
    def halves(x):
        x = x.astype(np.float32)
        high = x.astype(jnp.bfloat16)
        return high, (x - high.astype(np.float32)).astype(jnp.bfloat16)
    return (*halves(first), *halves(second), (c * scale).astype(np.float32), (s * scale).astype(np.float32))


def image_kernel(edges, x_ref, f_hi, f_lo, s_hi, s_lo, tw_c, tw_s, out_ref, z_ref):
    tiles = x_ref.shape[0] // 16
    inner = tw_c.shape[1]

    def product(high, low, x, dims):
        xh, xl = split(x)
        dot = lambda a, b: lax.dot_general(a, b, dims, preferred_element_type=f32)
        return dot(high, xh) + dot(high, xl) + dot(low, xh)

    columns = []
    for line in range(2):
        stack = []
        for p in range(2):
            for h in range(2):
                stack.append(jnp.concatenate(
                    [x_ref[pl.ds(line * 8 + p * 4 + 2 * h + j, tiles, stride=16), :] for j in range(2)], axis=1))
        columns.append(jnp.concatenate(stack, axis=0))
    x = jnp.concatenate(columns, axis=1)
    g = product(f_hi[...], f_lo[...], x, (((1,), (0,)), ((), ())))
    rows = []
    for line in range(2):
        real = g[:LANES, line * inner:(line + 1) * inner]
        imag = g[LANES:, line * inner:(line + 1) * inner]
        c, s = tw_c[...], tw_s[...]
        rows.append(jnp.concatenate([real * c - imag * s, real * s + imag * c], axis=1))
    z_ref[...] = product(s_hi[...], s_lo[...], jnp.concatenate(rows, axis=0), (((1,), (1,)), ((), ())))

    step = 16
    chunk = step * LANES
    cell = (lax.broadcasted_iota(jnp.int32, (step, LANES), 0) * LANES
            + lax.broadcasted_iota(jnp.int32, (step, LANES), 1))

    for line in range(2):
        lower, upper = edges[line, 0], edges[line, 1]
        span = (upper - lower).astype(f32)
        at = pl.ds(line * LANES, LANES)

        def basis(i):
            n = cell + i * chunk
            inside = (n >= lower) & (n < upper)
            xi = jnp.where(inside, -1.0 + (2.0 * (n - lower).astype(f32) + 1.0) / span, 0.0)
            polys = [jnp.ones_like(xi), 4.0 * xi]
            for k in range(1, GORDER - 1):
                polys.append((2.0 * (k + 2) * xi * polys[k] - (k + 3) * polys[k - 1]) / (k + 1))
            return inside, xi, polys

        def gather(i, sums):
            inside, xi, polys = basis(i)
            base = 1.0 - xi * xi
            weight = jnp.where(inside, base * jnp.sqrt(base), 0.0)
            field = [z_ref[pl.ds(c * inner + i * step, step), at] for c in range(2)]
            out = []
            for k in range(GORDER):
                w = weight * polys[k]
                out += [sums[3 * k] + w * field[0], sums[3 * k + 1] + w * field[1], sums[3 * k + 2] + w * polys[k]]
            return tuple(out)

        begin, end = lower // chunk, (upper + chunk - 1) // chunk
        zero = jnp.zeros((step, LANES), f32)
        sums = lax.fori_loop(begin, end, gather, (zero,) * (3 * GORDER))
        total = [jnp.sum(jnp.sum(v, axis=0, keepdims=True), axis=1, keepdims=True) for v in sums]
        coef = [(total[3 * k] / total[3 * k + 2], total[3 * k + 1] / total[3 * k + 2]) for k in range(GORDER)]

        def rebuild(i, carry):
            inside, xi, polys = basis(i)
            for c in range(2):
                rebuilt = coef[0][c] * polys[0]
                for k in range(1, GORDER):
                    rebuilt = rebuilt + coef[k][c] * polys[k]
                rows = pl.ds(c * inner + i * step, step)
                z_ref[rows, at] = jnp.where(inside, rebuilt, z_ref[rows, at])
            return carry
        lax.fori_loop(begin, end, rebuild, 0)
        for c in range(2):
            out_ref[c, pl.ds(line, inner, stride=2), :] = z_ref[c * inner:(c + 1) * inner, at]


def image(edges, x, width):
    tiles = x.shape[0] // 16
    inner = width // LANES
    consts = [jnp.asarray(t) for t in tables(tiles, width)]
    out = pl.pallas_call(
        image_kernel,
        in_specs=[pl.BlockSpec(memory_space=pltpu.SMEM)] + [vmem()] * 7,
        out_specs=vmem(),
        out_shape=jax.ShapeDtypeStruct((2, 2 * inner, LANES), f32),
        scratch_shapes=[pltpu.VMEM((2 * inner, 2 * LANES), f32)],
        compiler_params=pltpu.CompilerParams(vmem_limit_bytes=12 << 20),
        name="image",
    )(edges, x, *consts)
    return out.reshape(2, inner, 2, LANES).transpose(0, 2, 1, 3).reshape(2, 2, width)


def swap(block, flip):
    return lax.ppermute(block, "aperture", [(i, i ^ flip) for i in range(4)])


def on_device(sectors, footprint, own_blocks, edge_blocks, edges):
    tiles = lax.axis_size("tile")
    foot = footprint[0].T
    cut = edge_blocks.shape[1]
    high, rim, spread = early_terms(sectors[0], foot, own_blocks, edge_blocks, cut)
    incoming = lax.ppermute(rim, "tile", [(i, i + 1) for i in range(tiles - 1)])
    ha = swap(jnp.stack([high[1, 0], high[2, 0]]), 1)
    hb = swap(jnp.stack([high[3, 1], high[2, 1]]), 3)
    low = late_terms(spread, foot, own_blocks, cut) + incoming
    la = swap(jnp.stack([low[1, 0], low[2, 0]]), 1)
    lb = swap(jnp.stack([low[3, 1], low[2, 1]]), 3)
    qa = swap(jnp.concatenate([low[3, 0] + la[1], high[3, 0] + ha[1]]), 3)
    qb = swap(jnp.concatenate([low[1, 1] + lb[1], high[1, 1] + hb[1]]), 1)
    q = jnp.stack([qa, qb])
    packed = pack(
        [low[0], jnp.stack([la[0], lb[0]]), q[:, :cut]],
        [high[0], jnp.stack([ha[0], hb[0]]), q[:, cut:]],
    )
    moved = lax.all_to_all(packed.reshape(tiles, 16, LANES), "tile", 0, 0, tiled=True)
    return image(edges, moved.reshape(tiles * 16, LANES), tiles * own_blocks.shape[1])


def solution(mesh):
    in_specs = (
        P("aperture", "tile", None, None, None),
        P("aperture", "tile", None),
        P(),
        P(),
        P(("aperture", "tile"), None),
    )
    out_specs = P(None, ("aperture", "tile"), None)
    return jax.shard_map(
        on_device, mesh=mesh, in_specs=in_specs, out_specs=out_specs, check_vma=False
    )
```

```python
import functools
import math

import jax
import jax.numpy as jnp
import numpy as np
from jax import lax
from jax.experimental import pallas as pl
from jax.experimental.pallas import tpu as pltpu
from jax.sharding import PartitionSpec as P

GORDER = 8
LANES = 128
f32, bf16 = jnp.float32, jnp.bfloat16


def vmem():
    return pl.BlockSpec(memory_space=pltpu.VMEM)


def aperture(foot):
    return lax.axis_index("aperture")


def live(foot, slots, blocks):
    count = jnp.int32(0)
    for s in range(slots):
        count = count + (foot[0, s] < blocks).astype(jnp.int32)
    return count


def early_kernel(cfg, foot, x_hbm, own_hbm, edge_hbm, high_ref, rim_ref, x_ref, sums, xs, owns, edges, wide0, wide1, wide2, wide3, sems, bsem):
    slots, blocks, begin, tall, erows = cfg
    me = aperture(foot)
    depth = x_hbm.shape[1] // 8
    count = live(foot, slots, blocks)

    def fetch(s):
        return pltpu.make_async_copy(x_hbm.at[s], xs.at[s], sems.at[s])

    def start(s):
        @pl.when(s < count)
        def _():
            fetch(s).start()

    def arrive(s):
        @pl.when(s < count)
        def _():
            fetch(s).wait()

    own_copy = pltpu.make_async_copy(own_hbm.at[:, pl.ds(begin, tall), :], owns.at[pl.ds(0, blocks)], bsem.at[0])
    edge_copy = pltpu.make_async_copy(edge_hbm, edges.at[pl.ds(0, blocks)], bsem.at[1])
    fetch(0).start()
    start(1)
    own_copy.start()
    edge_copy.start()
    for s in range(2, 4):
        start(s)
    owns[blocks] = jnp.zeros((tall, depth), bf16)
    edges[blocks] = jnp.zeros((erows, depth), bf16)
    sums[...] = jnp.zeros_like(sums)

    def widen(s, wide):
        wide[...] = xs[jnp.minimum(s, count - 1)].astype(f32)

    def kernels(s):
        at = jnp.minimum(s, count - 1)
        o, e = foot[0, at], foot[1, at]
        own = owns[jnp.where(s < count, o, blocks)]
        edge = edges[jnp.where(s < count, e, blocks)]
        return jnp.concatenate([own, edge], axis=0)

    def columns(p, wide):
        return jnp.concatenate([wide[pl.ds(2 * j + p, depth, stride=8), :].astype(bf16) for j in range(4)], axis=1)

    def multiply(s, first, second):
        ka, kb = kernels(s), kernels(s + 1)
        for p in range(2):
            xa, xb = columns(p, first), columns(p, second)
            x_ref[s, p] = xa
            x_ref[s + 1, p] = xb
            y = jnp.dot(ka, xa, preferred_element_type=f32) + jnp.dot(kb, xb, preferred_element_type=f32)
            sums[p] += y

    fetch(0).wait()
    widen(0, wide0)
    arrive(1)
    widen(1, wide1)
    own_copy.wait()
    edge_copy.wait()
    for s in range(4, slots):
        start(s)

    def step(s, here, there):
        arrive(s + 2)
        arrive(s + 3)
        widen(s + 2, there[0])
        widen(s + 3, there[1])
        multiply(s, *here)

    def quad(t, carry):
        step(4 * t, (wide0, wide1), (wide2, wide3))

        @pl.when(4 * t + 2 < count)
        def _():
            step(4 * t + 2, (wide2, wide3), (wide0, wide1))
        return carry
    lax.fori_loop(0, (count + 3) // 4, quad, 0)
    for p in range(2):
        for j in range(4):
            high_ref[me ^ j, p] = sums[p, :tall, j * LANES:(j + 1) * LANES]
            rim_ref[me ^ j, p] = sums[p, tall:, j * LANES:(j + 1) * LANES]


def early_terms(sectors, foot, own, edge, begin):
    slots, depth, parts, lines = sectors.shape
    blocks, rows, _ = own.shape
    tall, erows = rows - begin, edge.shape[1]
    quarter = lines // 4
    sectors = sectors.reshape(slots, depth, 2, 4, LANES).transpose(0, 1, 3, 2, 4).reshape(slots, depth * 8, LANES)
    hbm = pl.BlockSpec(memory_space=pltpu.HBM)
    return pl.pallas_call(
        functools.partial(early_kernel, (slots, blocks, begin, tall, erows)),
        in_specs=[pl.BlockSpec(memory_space=pltpu.SMEM), hbm, hbm, hbm],
        out_specs=[vmem()] * 3,
        out_shape=[jax.ShapeDtypeStruct((4, 2, r, quarter), f32) for r in (tall, erows)]
        + [jax.ShapeDtypeStruct((slots, 2, depth, lines), bf16)],
        scratch_shapes=[
            pltpu.VMEM((2, tall + erows, lines), f32),
            pltpu.VMEM((slots, depth * 8, LANES), bf16),
            pltpu.VMEM((blocks + 1, tall, depth), bf16),
            pltpu.VMEM((blocks + 1, erows, depth), bf16),
            *[pltpu.VMEM((depth * 8, LANES), f32)] * 4,
            pltpu.SemaphoreType.DMA((slots,)),
            pltpu.SemaphoreType.DMA((2,)),
        ],
        compiler_params=pltpu.CompilerParams(vmem_limit_bytes=38 << 20),
        cost_estimate=pl.CostEstimate(
            flops=4 * slots * depth * lines * (tall + erows), bytes_accessed=slots * depth * lines * 4, transcendentals=0
        ),
        name="early_terms",
    )(pltpu.with_memory_space_constraint(foot, pltpu.HBM), *[pltpu.with_memory_space_constraint(v, pltpu.HBM) for v in (sectors, own, edge)])


def late_kernel(cfg, foot, x_ref, own_ref, low_ref, sums):
    slots, blocks, tall = cfg
    me = aperture(foot)
    count = live(foot, slots, blocks)
    sums[...] = jnp.zeros_like(sums)

    def add(s, ops):
        for p in range(2):
            y = sum(jnp.dot(own_ref[foot[0, s + i], :tall], x_ref[s + i, p], preferred_element_type=f32) for i in ops)
            sums[p] += y

    def pair(t, carry):
        add(2 * t, (0, 1))
        return carry
    lax.fori_loop(0, count // 2, pair, 0)

    @pl.when(count % 2 == 1)
    def _():
        add(count - 1, (0,))
    for p in range(2):
        for j in range(4):
            low_ref[me ^ j, p] = sums[p, :, j * LANES:(j + 1) * LANES]


def late_terms(x, foot, own, tall):
    slots, parts, depth, lines = x.shape
    blocks = own.shape[0]
    return pl.pallas_call(
        functools.partial(late_kernel, (slots, blocks, tall)),
        in_specs=[pl.BlockSpec(memory_space=pltpu.SMEM), vmem(), vmem()],
        out_specs=vmem(),
        out_shape=jax.ShapeDtypeStruct((4, 2, tall, lines // 4), f32),
        scratch_shapes=[pltpu.VMEM((2, tall, lines), f32)],
        compiler_params=pltpu.CompilerParams(vmem_limit_bytes=24 << 20),
        cost_estimate=pl.CostEstimate(
            flops=4 * slots * depth * lines * tall, bytes_accessed=slots * depth * lines * 4, transcendentals=0
        ),
        name="late_terms",
    )(pltpu.with_memory_space_constraint(foot, pltpu.HBM), x, own)


def pack_kernel(lows, *refs):
    *terms, out_ref = refs
    for p in range(2):
        row = 4 * p
        for group in (terms[:lows], terms[lows:]):
            for j in range(group[0].shape[1] // LANES):
                at = pl.ds(j * LANES, LANES)
                out_ref[pl.ds(row, LANES, stride=8), :] = sum(term[p, at] for term in group).T
                row += 1


def pack(low, high):
    return pl.pallas_call(
        functools.partial(pack_kernel, len(low)),
        in_specs=[vmem()] * (len(low) + len(high)),
        out_specs=vmem(),
        out_shape=jax.ShapeDtypeStruct((8 * LANES, LANES), f32),
        compiler_params=pltpu.CompilerParams(vmem_limit_bytes=8 << 20),
        name="pack",
    )(*low, *high)


def split(x):
    high = x.astype(bf16)
    return high, (x - high.astype(f32)).astype(bf16)


def tables(tiles, width):
    inner = width // LANES
    def wave(a, b, n):
        angle = 2.0 * math.pi / n * ((np.asarray(a)[:, None] * np.asarray(b)[None, :]) % n)
        return np.cos(angle), np.sin(angle)
    a = np.concatenate([2 * np.arange(tiles), 2 * np.arange(tiles) + 1])
    c, s = wave(np.arange(LANES), a, LANES)
    first = np.block([[c, -s], [s, c]])
    c, s = wave(np.arange(inner), np.arange(inner), inner)
    second = np.block([[c, -s], [s, c]])
    c, s = wave(np.arange(LANES), np.arange(inner), width)
    scale = 1.0 / math.sqrt(width)
    def halves(x):
        x = x.astype(np.float32)
        high = x.astype(jnp.bfloat16)
        return high, (x - high.astype(np.float32)).astype(jnp.bfloat16)
    return (*halves(first), *halves(second), (c * scale).astype(np.float32), (s * scale).astype(np.float32))


def image_kernel(edges, x_ref, f_hi, f_lo, s_hi, s_lo, tw_c, tw_s, out_ref, z_ref):
    tiles = x_ref.shape[0] // 16
    inner = tw_c.shape[1]

    def product(high, low, x, dims):
        xh, xl = split(x)
        dot = lambda a, b: lax.dot_general(a, b, dims, preferred_element_type=f32)
        return dot(high, xh) + dot(high, xl) + dot(low, xh)

    columns = []
    for line in range(2):
        stack = []
        for p in range(2):
            for h in range(2):
                stack.append(jnp.concatenate(
                    [x_ref[pl.ds(line * 8 + p * 4 + 2 * h + j, tiles, stride=16), :] for j in range(2)], axis=1))
        columns.append(jnp.concatenate(stack, axis=0))
    x = jnp.concatenate(columns, axis=1)
    g = product(f_hi[...], f_lo[...], x, (((1,), (0,)), ((), ())))
    rows = []
    for line in range(2):
        real = g[:LANES, line * inner:(line + 1) * inner]
        imag = g[LANES:, line * inner:(line + 1) * inner]
        c, s = tw_c[...], tw_s[...]
        rows.append(jnp.concatenate([real * c - imag * s, real * s + imag * c], axis=1))
    z_ref[...] = product(s_hi[...], s_lo[...], jnp.concatenate(rows, axis=0), (((1,), (1,)), ((), ())))

    step = 16
    chunk = step * LANES
    cell = (lax.broadcasted_iota(jnp.int32, (step, LANES), 0) * LANES
            + lax.broadcasted_iota(jnp.int32, (step, LANES), 1))

    for line in range(2):
        lower, upper = edges[line, 0], edges[line, 1]
        span = (upper - lower).astype(f32)
        at = pl.ds(line * LANES, LANES)

        def basis(i):
            n = cell + i * chunk
            inside = (n >= lower) & (n < upper)
            xi = jnp.where(inside, -1.0 + (2.0 * (n - lower).astype(f32) + 1.0) / span, 0.0)
            polys = [jnp.ones_like(xi), 4.0 * xi]
            for k in range(1, GORDER - 1):
                polys.append((2.0 * (k + 2) * xi * polys[k] - (k + 3) * polys[k - 1]) / (k + 1))
            return inside, xi, polys

        def gather(i, sums):
            inside, xi, polys = basis(i)
            base = 1.0 - xi * xi
            weight = jnp.where(inside, base * jnp.sqrt(base), 0.0)
            field = [z_ref[pl.ds(c * inner + i * step, step), at] for c in range(2)]
            out = []
            for k in range(GORDER):
                w = weight * polys[k]
                out += [sums[3 * k] + w * field[0], sums[3 * k + 1] + w * field[1], sums[3 * k + 2] + w * polys[k]]
            return tuple(out)

        begin, end = lower // chunk, (upper + chunk - 1) // chunk
        zero = jnp.zeros((step, LANES), f32)
        sums = lax.fori_loop(begin, end, gather, (zero,) * (3 * GORDER))
        total = [jnp.sum(jnp.sum(v, axis=0, keepdims=True), axis=1, keepdims=True) for v in sums]
        coef = [(total[3 * k] / total[3 * k + 2], total[3 * k + 1] / total[3 * k + 2]) for k in range(GORDER)]

        def rebuild(i, carry):
            inside, xi, polys = basis(i)
            for c in range(2):
                rebuilt = coef[0][c] * polys[0]
                for k in range(1, GORDER):
                    rebuilt = rebuilt + coef[k][c] * polys[k]
                rows = pl.ds(c * inner + i * step, step)
                z_ref[rows, at] = jnp.where(inside, rebuilt, z_ref[rows, at])
            return carry
        lax.fori_loop(begin, end, rebuild, 0)
        for c in range(2):
            out_ref[c, pl.ds(line, inner, stride=2), :] = z_ref[c * inner:(c + 1) * inner, at]


def image(edges, x, width):
    tiles = x.shape[0] // 16
    inner = width // LANES
    consts = [jnp.asarray(t) for t in tables(tiles, width)]
    out = pl.pallas_call(
        image_kernel,
        in_specs=[pl.BlockSpec(memory_space=pltpu.SMEM)] + [vmem()] * 7,
        out_specs=vmem(),
        out_shape=jax.ShapeDtypeStruct((2, 2 * inner, LANES), f32),
        scratch_shapes=[pltpu.VMEM((2 * inner, 2 * LANES), f32)],
        compiler_params=pltpu.CompilerParams(vmem_limit_bytes=12 << 20),
        name="image",
    )(edges, x, *consts)
    return out.reshape(2, inner, 2, LANES).transpose(0, 2, 1, 3).reshape(2, 2, width)


def swap(block, flip):
    return lax.ppermute(block, "aperture", [(i, i ^ flip) for i in range(4)])


def on_device(sectors, footprint, own_blocks, edge_blocks, edges):
    tiles = lax.axis_size("tile")
    foot = footprint[0].T
    cut = edge_blocks.shape[1]
    high, rim, spread = early_terms(sectors[0], foot, own_blocks, edge_blocks, cut)
    incoming = lax.ppermute(rim, "tile", [(i, i + 1) for i in range(tiles - 1)])
    ha = swap(jnp.stack([high[1, 0], high[2, 0]]), 1)
    hb = swap(jnp.stack([high[3, 1], high[2, 1]]), 3)
    low = late_terms(spread, foot, own_blocks, cut) + incoming
    qa, qb = swap(high[3, 0] + ha[1], 3), swap(high[1, 1] + hb[1], 1)
    packed = pack(
        [low[0]] + [swap(low[r], r) for r in (1, 3, 2)],
        [high[0], jnp.stack([ha[0], hb[0]]), jnp.stack([qa, qb])],
    )
    moved = lax.all_to_all(packed.reshape(tiles, 16, LANES), "tile", 0, 0, tiled=True)
    return image(edges, moved.reshape(tiles * 16, LANES), tiles * own_blocks.shape[1])


def solution(mesh):
    in_specs = (
        P("aperture", "tile", None, None, None),
        P("aperture", "tile", None),
        P(),
        P(),
        P(("aperture", "tile"), None),
    )
    out_specs = P(None, ("aperture", "tile"), None)
    return jax.shard_map(
        on_device, mesh=mesh, in_specs=in_specs, out_specs=out_specs, check_vma=False
    )
```
